32 devices in a mesh: head: 4 (over y, core), seq: 8 (over z, x).
Axes of the slice: x: 2, y: 2, z: 4, core: 2. Of those that a mesh axis runs over, the one named last changes fastest.
Arguments:
- queries: bfloat16 [2, 4, 32, 128], P(None, None, ('head', 'seq')), may hold values from -16 to 16
- keys: bfloat16 [2, 4, 16384, 128], P(None, 'head', 'seq'), may hold values from -6 to 6
- values: bfloat16 [2, 4, 16384, 128], P(None, 'head', 'seq'), may hold values from -6 to 6
- indices: int32 [4, 8, 1024], P('head'), may hold values from 0 to 16383, as said below
- sizes: int32 [4, 8], P('head'), may hold values from 128 to 1024, as said below
- owners: int32 [4, 8], P('head'), may hold values from 0 to 7, as said below
Outputs:
- compact_values: bfloat16 [4, 24, 1024, 128], P('head', 'seq')
The draws below stay inside these ranges and needn't reach their ends.
Inputs may be any that keep to these rules, and one draw needn't show every extreme that they name: `indices`: in each row of a head and fit, the 1024 positions are distinct and the first two are 0 and 1; only the first sizes[h,f] are used. `sizes`: multiples of 128; in each head one fit has 1024. `owners`: no index owns more than 3 fits of a head; in each head one index owns exactly 3.
All inputs are finite; a program needn't handle non-finite values.
Results may differ from the reference program's by a relative error of at most 0.008.
Values may be sent and summed in bfloat16 or wider, within the bound.
A program may use at most 128 MiB of HBM per device.

```python
import jax
import jax.numpy as jnp
from jax import lax

HD = 128
LAYERS = 2
FITS_LAYER = 4
CMAX = 1024
SLOTS = 3
KVH = 4
SEQ_LEN = 16384
QUERIES = 32
FITS = 8
STEP = 128
N_SEQ = 8


def draw_keys(key, part):
    base = jax.random.normal(jax.random.fold_in(key, 1), (LAYERS, KVH, SEQ_LEN, HD), jnp.float32)
    return jnp.clip(base, -6.0, 6.0).astype(jnp.bfloat16)


def draw_queries(key, part):
    base = 2.5 * jax.random.normal(jax.random.fold_in(key, 3), (LAYERS, KVH, QUERIES, HD), jnp.float32)
    return jnp.clip(base, -16.0, 16.0).astype(jnp.bfloat16)


def draw_indices(key, part):
    streams = jax.random.split(jax.random.fold_in(key, 6), KVH * FITS)
    picked = jax.vmap(lambda one: jax.random.permutation(one, SEQ_LEN - 2)[:CMAX - 2] + 2)(streams)
    lead = jnp.broadcast_to(jnp.array([0, 1], jnp.int32), (KVH * FITS, 2))
    return jnp.concatenate([lead, picked.astype(jnp.int32)], axis=1).reshape(KVH, FITS, CMAX)


def draw_sizes(key, part):
    units = jax.random.randint(jax.random.fold_in(key, 7), (KVH, FITS), 1, 9)
    chosen = jax.random.randint(jax.random.fold_in(key, 8), (KVH, 1), 0, FITS)
    units = jnp.where(jnp.arange(FITS)[None, :] == chosen, 8, units)
    return (units * STEP).astype(jnp.int32)


def owner_row(one):
    busy = jax.random.randint(jax.random.fold_in(one, 1), (), 0, N_SEQ)
    rest = jax.random.permutation(jax.random.fold_in(one, 2), N_SEQ - 1)
    rest = jnp.where(rest >= busy, rest + 1, rest)[:FITS - SLOTS]
    listed = jnp.concatenate([jnp.full((SLOTS,), busy), rest])
    order = jax.random.permutation(jax.random.fold_in(one, 3), FITS)
    return listed[order].astype(jnp.int32)


def draw_owners(key, part):
    streams = jax.random.split(jax.random.fold_in(key, 9), KVH)
    return jax.vmap(owner_row)(streams)


def levels(own_key, extent, shards, low, top_value):
    level, own = 1.0, jax.random.fold_in(own_key, 6)
    for position, shards_of in shards:
        draws = jnp.exp(jax.random.uniform(jax.random.fold_in(own, position), (shards_of,), jnp.float32, low / len(shards), top_value / len(shards)))
        level = level * jnp.repeat(draws, extent[position] // shards_of).reshape([-1 if axis == position else 1 for axis in range(len(extent))])
    return level


def noise(own_key, shape, scale, limit, cuts=(), kind=jnp.bfloat16):
    entries = scale * jax.random.normal(own_key, shape, jnp.float32)
    if cuts:
        entries = entries * levels(own_key, shape, cuts, -0.22, 0.18)
    return jnp.clip(entries, -limit, limit).astype(kind)


def setup_inputs(seed: int = 0) -> dict:
    splits = jax.random.split(jax.random.key(seed), 7)
    queries = draw_queries(jax.random.fold_in(splits[6], 71), 0)
    keys = draw_keys(jax.random.fold_in(splits[6], 71), 0)
    values = noise(splits[2], (LAYERS, KVH, SEQ_LEN, HD), 1.0, 6.0, ((1, 4), (2, 8)))
    indices = draw_indices(jax.random.fold_in(splits[6], 71), 0)
    sizes = draw_sizes(jax.random.fold_in(splits[6], 71), 0)
    owners = draw_owners(jax.random.fold_in(splits[6], 71), 0)
    return {"queries": queries, "keys": keys, "values": values, "indices": indices, "sizes": sizes, "owners": owners}


RIDGE = 0.3

def solve_fit(query_rows, target_rows, compact, size):
    scale = query_rows.shape[-1] ** (-0.5)
    width = compact.shape[0]
    scores = lax.dot_general(query_rows.astype(jnp.float32), compact.astype(jnp.float32), (((1,), (1,)), ((), ())), preferred_element_type=jnp.float32) * scale
    live = jnp.arange(width, dtype=jnp.int32) < size
    scores = jnp.where(live[None, :], scores, -jnp.inf)
    peak = jnp.max(scores, axis=1)
    expo = jnp.exp(scores - peak[:, None])
    probs = (expo / jnp.sum(expo, axis=1)[:, None]).astype(jnp.bfloat16)
    gram = lax.dot_general(probs.astype(jnp.float32), probs.astype(jnp.float32), (((0,), (0,)), ((), ())), preferred_element_type=jnp.float32)
    rhs = lax.dot_general(probs.astype(jnp.float32), target_rows.astype(jnp.float32), (((0,), (0,)), ((), ())), preferred_element_type=jnp.float32)
    ridge = RIDGE * jnp.trace(gram) / size.astype(jnp.float32)
    system = gram + jnp.diag(jnp.where(live, ridge, jnp.float32(1.0)))
    factor = jnp.linalg.cholesky(system)
    solution = jax.scipy.linalg.cho_solve((factor, True), rhs)
    return solution.astype(jnp.bfloat16)

def attend(query_rows, key_rows, value_rows):
    scale = query_rows.shape[-1] ** (-0.5)
    scores = jnp.dot(query_rows.astype(jnp.float32), key_rows.astype(jnp.float32).T.astype(jnp.float32), preferred_element_type=jnp.float32) * scale
    peak = jnp.max(scores, axis=1)
    weights = jnp.exp(scores - peak[:, None])
    total = jnp.sum(weights, axis=1)
    rounded = lax.optimization_barrier(weights.astype(jnp.bfloat16))
    numer = jnp.dot(rounded.astype(jnp.float32), value_rows.astype(jnp.float32), preferred_element_type=jnp.float32)
    return (numer / total[:, None]).astype(jnp.bfloat16)

def reference(queries, keys, values, indices, sizes, owners):
    layers, heads = (keys.shape[0], keys.shape[1])
    width = keys.shape[3]
    flat_q = queries.reshape(layers * heads, QUERIES, width)
    flat_k = keys.reshape(layers * heads, SEQ_LEN, width)
    flat_v = values.reshape(layers * heads, SEQ_LEN, width)
    targets = lax.map(lambda group: attend(group[0], group[1], group[2]), (flat_q, flat_k, flat_v))
    targets = targets.reshape(layers, heads, QUERIES, width)
    head_ids = jnp.repeat(jnp.arange(heads, dtype=jnp.int32), FITS)
    fit_list = jnp.tile(jnp.arange(FITS, dtype=jnp.int32), heads)

    def one_fit(pair):
        head, fit = pair
        layer = fit // FITS_LAYER
        compact = jnp.take(keys[layer, head], indices[head, fit], axis=0)
        return solve_fit(queries[layer, head], targets[layer, head], compact, sizes[head, fit])
    solutions = lax.map(one_fit, (head_ids, fit_list)).reshape(heads, FITS, CMAX, width)
    fit_ids = jnp.arange(FITS, dtype=jnp.int32)
    same = owners[:, :, None] == owners[:, None, :]
    before = fit_ids[:, None] > fit_ids[None, :]
    earlier = jnp.sum((same & before[None]).astype(jnp.int32), axis=2)
    slot = (owners * SLOTS + earlier).astype(jnp.int32)
    result = jnp.zeros((heads, N_SEQ * SLOTS, CMAX, width), jnp.bfloat16)
    return result.at[jnp.arange(heads, dtype=jnp.int32)[:, None], slot].set(solutions)
```

```python
import functools

import jax
import jax.numpy as jnp
from jax import lax
from jax.experimental import pallas as pl
from jax.experimental.pallas import tpu as pltpu
from jax.sharding import PartitionSpec as P

FITS_LAYER = 4
SLOTS = 3
RIDGE = 0.3
LANES = 128
FAR = -1e30

NT = (((1,), (1,)), ((), ()))
TN = (((0,), (0,)), ((), ()))


def attend_kernel(sizes_ref, q_ref, k_ref, v_ref, idx_ref, e_ref, aux_ref, s_ref, g_ref):
    layers, rows, width = q_ref.shape
    local_len = k_ref.shape[1]
    fits, capacity = idx_ref.shape
    start = lax.axis_index("seq") * local_len
    lane = lax.broadcasted_iota(jnp.int32, (rows, LANES), 1)
    scale = width ** (-0.5)
    for layer in range(layers):
        scores = (
            lax.dot_general(q_ref[layer], k_ref[layer], NT, preferred_element_type=jnp.float32)
            * scale
        )
        s_ref[layer] = scores
        peak = jnp.max(scores, axis=1, keepdims=True)
        weights = jnp.exp(scores - peak)
        total = jnp.sum(weights, axis=1, keepdims=True)
        numer = jnp.dot(
            weights.astype(jnp.bfloat16), v_ref[layer], preferred_element_type=jnp.float32
        )
        side = jnp.where(lane < 32, total, peak)
        for fit in range(layer * FITS_LAYER, (layer + 1) * FITS_LAYER):
            aux_ref[fit, 0] = numer
            aux_ref[fit, 1] = side

    def one_fit(fit, carry):
        layer = fit // FITS_LAYER
        size = sizes_ref[0, fit]

        def one_tile(tile, top):
            base = pl.multiple_of(tile * LANES, LANES)
            drawn = idx_ref[:, pl.ds(base, LANES)]
            mine = lax.broadcasted_iota(jnp.int32, (fits, LANES), 0) == fit
            offset = jnp.sum(jnp.where(mine, drawn, 0), axis=0, keepdims=True) - start
            column = base + lax.broadcasted_iota(jnp.int32, (1, LANES), 1)
            inside = (offset >= 0) & (offset < local_len) & (column < size)
            offset = jnp.broadcast_to(jnp.where(inside, offset, -1), (rows, LANES))
            high = offset >> 7
            low = offset & (LANES - 1)
            picked = jnp.full((rows, LANES), FAR, jnp.float32)
            for block in range(local_len // LANES):
                part = s_ref[layer, :, block * LANES : (block + 1) * LANES]
                found = jnp.take_along_axis(part, low, axis=1, mode="promise_in_bounds")
                picked = jnp.where(high == block, found, picked)
            g_ref[:, pl.ds(base, LANES)] = picked
            return jnp.maximum(top, jnp.max(picked, axis=1, keepdims=True))

        top = lax.fori_loop(
            0, capacity // LANES, one_tile, jnp.full((rows, 1), FAR, jnp.float32)
        )
        picked = g_ref[...]
        expo = jnp.where(picked > 0.5 * FAR, jnp.exp(picked - top), 0.0)
        e_ref[fit] = expo.astype(jnp.bfloat16)
        aux_ref[fit, 1] = jnp.where(lane < 64, aux_ref[fit, 1], top)
        return carry

    lax.fori_loop(0, fits, one_fit, 0)


def solve_rows(system, target):
    rows = system.shape[0]
    row = lax.broadcasted_iota(jnp.int32, (rows, 1), 0)
    if rows <= 64:
        for k in range(rows):
            inverse = 1.0 / system[k : k + 1, k : k + 1]
            pivot_s = system[k : k + 1, :] * inverse
            pivot_t = target[k : k + 1, :] * inverse
            column = jnp.where(row == k, system[:, k : k + 1] - 1.0, system[:, k : k + 1])
            system = system - column * pivot_s
            target = target - column * pivot_t
        return target
    lane = lax.broadcasted_iota(jnp.int32, (1, rows), 1)

    def step(k, state):
        system, target = state
        column = jnp.sum(jnp.where(lane == k, system, 0.0), axis=1, keepdims=True)
        here = row == k
        inverse = 1.0 / jnp.sum(jnp.where(here, column, 0.0), axis=0, keepdims=True)
        pivot_s = jnp.sum(jnp.where(here, system, 0.0), axis=0, keepdims=True) * inverse
        pivot_t = jnp.sum(jnp.where(here, target, 0.0), axis=0, keepdims=True) * inverse
        column = jnp.where(here, column - 1.0, column)
        return system - column * pivot_s, target - column * pivot_t

    return lax.fori_loop(0, rows, step, (system, target))[1]


def merge_fit(e_at, aux_at, groups, size):
    first = aux_at(0, 1)
    peak, top = first[:, 32:33], first[:, 64:65]
    for source in range(1, groups):
        side = aux_at(source, 1)
        peak = jnp.maximum(peak, side[:, 32:33])
        top = jnp.maximum(top, side[:, 64:65])
    numer, total, probs = 0.0, 0.0, 0.0
    for source in range(groups):
        side = aux_at(source, 1)
        factor = jnp.exp(side[:, 32:33] - peak)
        numer = numer + aux_at(source, 0) * factor
        total = total + side[:, 0:1] * factor
        probs = probs + e_at(source).astype(jnp.float32) * jnp.exp(side[:, 64:65] - top)
    target = (numer / total).astype(jnp.bfloat16).astype(jnp.float32)
    probs = probs / jnp.sum(probs, axis=1, keepdims=True)
    return probs.astype(jnp.bfloat16), target


def fit_rows(probs, target, size):
    rows = probs.shape[0]
    gram = lax.dot_general(probs, probs, NT, preferred_element_type=jnp.float32)
    diagonal = lax.broadcasted_iota(jnp.int32, (rows, rows), 0) == lax.broadcasted_iota(
        jnp.int32, (rows, rows), 1
    )
    trace = jnp.sum(jnp.where(diagonal, gram, 0.0))
    ridge = RIDGE * trace / size
    return solve_rows(jnp.where(diagonal, gram + ridge, gram), target)


def solve_kernel(sizes_ref, e_ref, aux_ref, p_ref, x_ref):
    groups = e_ref.shape[0]
    fits = sizes_ref.shape[1]
    fit = jnp.minimum(lax.axis_index("seq"), fits - 1)
    size = sizes_ref[0, fit].astype(jnp.float32)
    probs, target = merge_fit(
        lambda s: e_ref[s], lambda s, part: aux_ref[s, part], groups, size
    )
    p_ref[...] = probs
    x_ref[...] = fit_rows(probs, target, size)


def place_kernel(slot_ref, p_ref, x_ref, out_ref):
    for slot in range(SLOTS):
        fit = slot_ref[0, slot]
        live = slot_ref[1, slot]

        @pl.when(live > 0)
        def _():
            probs = p_ref[fit]
            rows = x_ref[fit]
            high = rows.astype(jnp.bfloat16)
            low = (rows - high.astype(jnp.float32)).astype(jnp.bfloat16)
            out_ref[0, slot] = lax.dot_general(
                jnp.concatenate([probs, probs], axis=0),
                jnp.concatenate([high, low], axis=0),
                TN,
                preferred_element_type=jnp.float32,
            ).astype(jnp.bfloat16)

        @pl.when(live == 0)
        def _():
            out_ref[0, slot] = jnp.zeros(out_ref.shape[2:], jnp.bfloat16)


VMEM = pl.BlockSpec(memory_space=pltpu.VMEM)
SMEM = pl.BlockSpec(memory_space=pltpu.SMEM)
PARAMS = dict(vmem_limit_bytes=60 * 1024 * 1024)


def on_device(queries, keys, values, indices, sizes, owners):
    regrouped = lax.all_to_all(queries, "head", split_axis=1, concat_axis=2, tiled=True)
    gathered = lax.all_gather(regrouped, "seq", axis=2, tiled=True)
    all_queries = gathered[:, 0]
    layers, rows, width = all_queries.shape
    key_rows = keys[:, 0]
    value_rows = values[:, 0]
    local_len = key_rows.shape[1]
    fits, capacity = indices.shape[1:]
    groups = lax.axis_size("seq")
    expo, aux = pl.pallas_call(
        attend_kernel,
        out_shape=(
            jax.ShapeDtypeStruct((fits, rows, capacity), jnp.bfloat16),
            jax.ShapeDtypeStruct((fits, 2, rows, width), jnp.float32),
        ),
        in_specs=[SMEM] + [VMEM] * 4,
        out_specs=(VMEM, VMEM),
        scratch_shapes=[
            pltpu.VMEM((layers, rows, local_len), jnp.float32),
            pltpu.VMEM((rows, capacity), jnp.float32),
        ],
        compiler_params=pltpu.CompilerParams(**PARAMS),
    )(sizes, all_queries, key_rows, value_rows, indices[0])
    if groups > fits:
        spare = groups - fits
        expo = jnp.pad(expo, ((0, spare), (0, 0), (0, 0)))
        aux = jnp.pad(aux, ((0, spare), (0, 0), (0, 0), (0, 0)))
    expo = lax.all_to_all(expo, "seq", split_axis=0, concat_axis=0, tiled=True)
    aux = lax.all_to_all(aux, "seq", split_axis=0, concat_axis=0, tiled=True)
    probs, solved = pl.pallas_call(
        solve_kernel,
        out_shape=(
            jax.ShapeDtypeStruct((rows, capacity), jnp.bfloat16),
            jax.ShapeDtypeStruct((rows, width), jnp.float32),
        ),
        in_specs=[SMEM] + [VMEM] * 2,
        out_specs=(VMEM, VMEM),
        compiler_params=pltpu.CompilerParams(**PARAMS),
    )(sizes, expo, aux)
    probs = lax.all_gather(probs, "seq")[:fits]
    solved = lax.all_gather(solved, "seq")[:fits]
    return place(owners, probs, solved, capacity)


def place(owners, probs, solved, capacity):
    width = solved.shape[-1]
    owned = owners[0]
    fits = owned.shape[0]
    fit_ids = jnp.arange(fits, dtype=jnp.int32)
    same = owned[:, None] == owned[None, :]
    earlier = jnp.sum((same & (fit_ids[:, None] > fit_ids[None, :])).astype(jnp.int32), axis=1)
    match = (owned == lax.axis_index("seq"))[None, :] & (
        earlier[None, :] == jnp.arange(SLOTS, dtype=jnp.int32)[:, None]
    )
    chosen = jnp.sum(jnp.where(match, fit_ids[None, :], 0), axis=1)
    live = jnp.any(match, axis=1).astype(jnp.int32)
    return pl.pallas_call(
        place_kernel,
        out_shape=jax.ShapeDtypeStruct((1, SLOTS, capacity, width), jnp.bfloat16),
        in_specs=[SMEM, VMEM, VMEM],
        out_specs=VMEM,
        compiler_params=pltpu.CompilerParams(**PARAMS),
    )(jnp.stack([chosen, live]), probs, solved)


def solution(mesh):
    in_specs = (
        P(None, None, ("head", "seq"), None),
        P(None, "head", "seq", None),
        P(None, "head", "seq", None),
        P("head", None, None),
        P("head", None),
        P("head", None),
    )
    out_specs = P("head", "seq", None, None)
    return jax.shard_map(
        on_device, mesh=mesh, in_specs=in_specs, out_specs=out_specs, check_vma=False
    )
```

```python
import jax
import jax.numpy as jnp
from jax import lax
from jax.experimental import pallas as pl
from jax.experimental.pallas import tpu as pltpu
from jax.sharding import PartitionSpec as P

FITS_LAYER = 4
SLOTS = 3
RIDGE = 0.3
LANES = 128
FAR = -1e30

SUBLANES = 8
MESH = pl.DeviceIdType.MESH
NT = (((1,), (1,)), ((), ()))
TN = (((0,), (0,)), ((), ()))


def attend_kernel(sizes_ref, q_ref, k_ref, v_ref, idx_ref, e_ref, aux_ref, s_ref, g_ref):
    layers, local_len, width = k_ref.shape
    rows = q_ref.shape[0] // SUBLANES
    fits, capacity = idx_ref.shape
    start = lax.axis_index("seq") * local_len
    lane = lax.broadcasted_iota(jnp.int32, (rows, LANES), 1)
    scale = width ** (-0.5)
    for layer in range(layers):
        query_rows = q_ref[pl.ds(layer, rows, stride=SUBLANES), :].astype(jnp.bfloat16)
        scores = (
            lax.dot_general(query_rows, k_ref[layer], NT, preferred_element_type=jnp.float32)
            * scale
        )
        s_ref[layer] = scores
        peak = jnp.max(scores, axis=1, keepdims=True)
        weights = jnp.exp(scores - peak)
        total = jnp.sum(weights, axis=1, keepdims=True)
        numer = jnp.dot(
            weights.astype(jnp.bfloat16), v_ref[layer], preferred_element_type=jnp.float32
        )
        side = jnp.where(lane < 32, total, peak)
        for fit in range(layer * FITS_LAYER, (layer + 1) * FITS_LAYER):
            aux_ref[fit, 0] = numer
            aux_ref[fit, 1] = side

    def one_fit(fit, carry):
        layer = fit // FITS_LAYER
        size = sizes_ref[0, fit]

        def one_tile(tile, top):
            base = pl.multiple_of(tile * LANES, LANES)
            drawn = idx_ref[:, pl.ds(base, LANES)]
            mine = lax.broadcasted_iota(jnp.int32, (fits, LANES), 0) == fit
            offset = jnp.sum(jnp.where(mine, drawn, 0), axis=0, keepdims=True) - start
            column = base + lax.broadcasted_iota(jnp.int32, (1, LANES), 1)
            inside = (offset >= 0) & (offset < local_len) & (column < size)
            offset = jnp.broadcast_to(jnp.where(inside, offset, -1), (rows, LANES))
            high = offset >> 7
            low = offset & (LANES - 1)
            picked = jnp.full((rows, LANES), FAR, jnp.float32)
            for block in range(local_len // LANES):
                part = s_ref[layer, :, block * LANES : (block + 1) * LANES]
                found = jnp.take_along_axis(part, low, axis=1, mode="promise_in_bounds")
                picked = jnp.where(high == block, found, picked)
            g_ref[:, pl.ds(base, LANES)] = picked
            return jnp.maximum(top, jnp.max(picked, axis=1, keepdims=True))

        top = lax.fori_loop(
            0, capacity // LANES, one_tile, jnp.full((rows, 1), FAR, jnp.float32)
        )
        picked = g_ref[...]
        expo = jnp.where(picked > 0.5 * FAR, jnp.exp(picked - top), 0.0)
        e_ref[fit] = expo.astype(jnp.bfloat16)
        aux_ref[fit, 1] = jnp.where(lane < 64, aux_ref[fit, 1], top)
        return carry

    lax.fori_loop(0, fits, one_fit, 0)


def solve_rows(system, target):
    rows = system.shape[0]
    row = lax.broadcasted_iota(jnp.int32, (rows, 1), 0)
    if rows <= 64:
        for k in range(rows):
            inverse = 1.0 / system[k : k + 1, k : k + 1]
            pivot_s = system[k : k + 1, :] * inverse
            pivot_t = target[k : k + 1, :] * inverse
            column = jnp.where(row == k, system[:, k : k + 1] - 1.0, system[:, k : k + 1])
            system = system - column * pivot_s
            target = target - column * pivot_t
        return target
    lane = lax.broadcasted_iota(jnp.int32, (1, rows), 1)

    def step(k, state):
        system, target = state
        column = jnp.sum(jnp.where(lane == k, system, 0.0), axis=1, keepdims=True)
        here = row == k
        inverse = 1.0 / jnp.sum(jnp.where(here, column, 0.0), axis=0, keepdims=True)
        pivot_s = jnp.sum(jnp.where(here, system, 0.0), axis=0, keepdims=True) * inverse
        pivot_t = jnp.sum(jnp.where(here, target, 0.0), axis=0, keepdims=True) * inverse
        column = jnp.where(here, column - 1.0, column)
        return system - column * pivot_s, target - column * pivot_t

    return lax.fori_loop(0, rows, step, (system, target))[1]


def merge_fit(e_at, aux_at, groups, size):
    first = aux_at(0, 1)
    peak, top = first[:, 32:33], first[:, 64:65]
    for source in range(1, groups):
        side = aux_at(source, 1)
        peak = jnp.maximum(peak, side[:, 32:33])
        top = jnp.maximum(top, side[:, 64:65])
    numer, total, probs = 0.0, 0.0, 0.0
    for source in range(groups):
        side = aux_at(source, 1)
        factor = jnp.exp(side[:, 32:33] - peak)
        numer = numer + aux_at(source, 0) * factor
        total = total + side[:, 0:1] * factor
        probs = probs + e_at(source).astype(jnp.float32) * jnp.exp(side[:, 64:65] - top)
    target = (numer / total).astype(jnp.bfloat16).astype(jnp.float32)
    probs = probs / jnp.sum(probs, axis=1, keepdims=True)
    return probs.astype(jnp.bfloat16), target


def fit_rows(probs, target, size):
    rows = probs.shape[0]
    gram = lax.dot_general(probs, probs, NT, preferred_element_type=jnp.float32)
    diagonal = lax.broadcasted_iota(jnp.int32, (rows, rows), 0) == lax.broadcasted_iota(
        jnp.int32, (rows, rows), 1
    )
    trace = jnp.sum(jnp.where(diagonal, gram, 0.0))
    ridge = RIDGE * trace / size
    return solve_rows(jnp.where(diagonal, gram + ridge, gram), target)


def enter(axes):
    barrier = pltpu.get_barrier_semaphore()
    total = 0
    for axis in axes:
        me, size = lax.axis_index(axis), lax.axis_size(axis)
        for step in range(1, size):
            pl.semaphore_signal(
                barrier, inc=1, device_id={axis: lax.rem(me + step, size)}, device_id_type=MESH
            )
        total += size - 1
    pl.semaphore_wait(barrier, total)


def send(source, target, send_sem, recv_sem, axis, peer):
    return pltpu.make_async_remote_copy(
        src_ref=source,
        dst_ref=target,
        send_sem=send_sem,
        recv_sem=recv_sem,
        device_id={axis: peer},
        device_id_type=MESH,
    )


def query_kernel(q_ref, out_ref, piece, column, table, send_head, recv_head, send_seq, recv_seq):
    layers, heads, count, width = q_ref.shape
    my_head, my_seq = lax.axis_index("head"), lax.axis_index("seq")
    groups = lax.axis_size("seq")
    for head in range(heads):
        for layer in range(layers):
            piece[head, layer : layer + 1, :] = q_ref[layer, head].astype(jnp.float32)
        piece[head, layers:, :] = jnp.zeros((SUBLANES - layers, width), jnp.float32)
    enter(("head", "seq"))
    column[0] = piece[my_head]
    copies = []
    for step in range(1, heads):
        peer = lax.rem(my_head + step, heads)
        copies.append(
            send(
                piece.at[peer],
                column.at[step],
                send_head.at[step],
                recv_head.at[step],
                "head",
                peer,
            )
        )
        copies[-1].start()
    for copy in copies:
        copy.wait_recv()
    later = []
    for step in range(1, groups):
        peer = lax.rem(my_seq + step, groups)
        later.append(
            send(column, table.at[my_seq], send_seq.at[step], recv_seq.at[step], "seq", peer)
        )
        later[-1].start()
    table[my_seq] = column[...]
    for copy in copies:
        copy.wait_send()
    for copy in later:
        copy.wait()
    out_ref[...] = table[...]


def solve_kernel(
    sizes_ref, e_ref, aux_ref, p_ref, x_ref,
    e_in, aux_in, p_all, x_all, p_mine, x_mine,
    send_in, recv_in, send_out, recv_out,
):
    groups = lax.axis_size("seq")
    me = lax.axis_index("seq")
    fits = sizes_ref.shape[1]
    fit = jnp.minimum(me, fits - 1)

    def only(condition, act):
        if groups <= fits:
            act()
        else:
            pl.when(condition)(act)

    def inbound(step):
        peer = lax.rem(me + step, groups)
        target = jnp.minimum(peer, fits - 1)
        return peer, [
            send(
                aux_ref.at[target], aux_in.at[step],
                send_in.at[0, step], recv_in.at[0, step], "seq", peer,
            ),
            send(
                e_ref.at[target], e_in.at[step],
                send_in.at[1, step], recv_in.at[1, step], "seq", peer,
            ),
        ]

    enter(("seq",))
    moves = [inbound(step) for step in range(1, groups)]
    for part in range(2):
        for peer, pair in moves:
            only(peer < fits, pair[part].start)
    aux_in[0] = aux_ref[fit]
    e_in[0] = e_ref[fit]

    outs = []
    for step in range(1, groups):
        peer = lax.rem(me + step, groups)
        outs.append(
            [
                send(
                    p_mine, p_all.at[fit],
                    send_out.at[0, step], recv_out.at[0, step], "seq", peer,
                ),
                send(
                    x_mine, x_all.at[fit],
                    send_out.at[1, step], recv_out.at[1, step], "seq", peer,
                ),
            ]
        )

    def work():
        for peer, pair in moves:
            pair[0].wait_recv()
        for peer, pair in moves:
            pair[1].wait_recv()
        size = sizes_ref[0, fit].astype(jnp.float32)
        probs, target = merge_fit(
            lambda s: e_in[s], lambda s, part: aux_in[s, part], groups, size
        )
        p_mine[...] = probs
        p_all[fit] = probs
        for pair in outs:
            pair[0].start()
        solved = fit_rows(probs, target, size)
        x_mine[...] = solved
        x_all[fit] = solved
        for pair in outs:
            pair[1].start()

    only(me < fits, work)
    for step in range(1, groups):
        source = lax.rem(me + groups - step, groups)
        for part in range(2):
            only(source < fits, outs[step - 1][part].wait_recv)
            only(me < fits, outs[step - 1][part].wait_send)
            only(moves[step - 1][0] < fits, moves[step - 1][1][part].wait_send)
    p_ref[...] = p_all[...]
    x_ref[...] = x_all[...]


def place_kernel(owners_ref, p_ref, x_ref, out_ref):
    me = lax.axis_index("seq")
    fits = p_ref.shape[0]
    count = jnp.int32(0)
    chosen = [jnp.int32(0)] * SLOTS
    for fit in range(fits):
        mine = owners_ref[0, fit] == me
        for slot in range(SLOTS):
            chosen[slot] = jnp.where(mine & (count == slot), fit, chosen[slot])
        count = count + mine.astype(jnp.int32)
    for slot in range(SLOTS):

        @pl.when(count > slot)
        def _():
            probs = p_ref[chosen[slot]]
            rows = x_ref[chosen[slot]]
            high = rows.astype(jnp.bfloat16)
            low = (rows - high.astype(jnp.float32)).astype(jnp.bfloat16)
            out_ref[0, slot] = lax.dot_general(
                jnp.concatenate([probs, probs], axis=0),
                jnp.concatenate([high, low], axis=0),
                TN,
                preferred_element_type=jnp.float32,
            ).astype(jnp.bfloat16)

        @pl.when(count <= slot)
        def _():
            out_ref[0, slot] = jnp.zeros(out_ref.shape[2:], jnp.bfloat16)


VMEM = pl.BlockSpec(memory_space=pltpu.VMEM)
SMEM = pl.BlockSpec(memory_space=pltpu.SMEM)
PARAMS = dict(vmem_limit_bytes=60 * 1024 * 1024)


def on_device(queries, keys, values, indices, sizes, owners):
    layers, heads, count, width = queries.shape
    groups = lax.axis_size("seq")
    rows = groups * heads * count
    local_len = keys.shape[2]
    fits, capacity = indices.shape[1:]
    dma = pltpu.SemaphoreType.DMA
    all_queries = pl.pallas_call(
        query_kernel,
        out_shape=jax.ShapeDtypeStruct((groups, heads, SUBLANES, width), jnp.float32),
        in_specs=[VMEM],
        out_specs=VMEM,
        scratch_shapes=[
            pltpu.VMEM((heads, SUBLANES, width), jnp.float32),
            pltpu.VMEM((heads, SUBLANES, width), jnp.float32),
            pltpu.VMEM((groups, heads, SUBLANES, width), jnp.float32),
            dma((heads,)),
            dma((heads,)),
            dma((groups,)),
            dma((groups,)),
        ],
        compiler_params=pltpu.CompilerParams(collective_id=1, has_side_effects=True, **PARAMS),
    )(queries)
    expo, aux = pl.pallas_call(
        attend_kernel,
        out_shape=(
            jax.ShapeDtypeStruct((fits, rows, capacity), jnp.bfloat16),
            jax.ShapeDtypeStruct((fits, 2, rows, width), jnp.float32),
        ),
        in_specs=[SMEM] + [VMEM] * 4,
        out_specs=(VMEM, VMEM),
        scratch_shapes=[
            pltpu.VMEM((layers, rows, local_len), jnp.float32),
            pltpu.VMEM((rows, capacity), jnp.float32),
        ],
        compiler_params=pltpu.CompilerParams(**PARAMS),
    )(
        sizes,
        all_queries.reshape(rows * SUBLANES, width),
        keys[:, 0],
        values[:, 0],
        indices[0],
    )
    probs, solved = pl.pallas_call(
        solve_kernel,
        out_shape=(
            jax.ShapeDtypeStruct((fits, rows, capacity), jnp.bfloat16),
            jax.ShapeDtypeStruct((fits, rows, width), jnp.float32),
        ),
        in_specs=[SMEM] + [VMEM] * 2,
        out_specs=(VMEM, VMEM),
        scratch_shapes=[
            pltpu.VMEM((groups, rows, capacity), jnp.bfloat16),
            pltpu.VMEM((groups, 2, rows, width), jnp.float32),
            pltpu.VMEM((fits, rows, capacity), jnp.bfloat16),
            pltpu.VMEM((fits, rows, width), jnp.float32),
            pltpu.VMEM((rows, capacity), jnp.bfloat16),
            pltpu.VMEM((rows, width), jnp.float32),
            dma((2, groups)),
            dma((2, groups)),
            dma((2, groups)),
            dma((2, groups)),
        ],
        compiler_params=pltpu.CompilerParams(collective_id=2, has_side_effects=True, **PARAMS),
    )(sizes, expo, aux)
    return pl.pallas_call(
        place_kernel,
        out_shape=jax.ShapeDtypeStruct((1, SLOTS, capacity, width), jnp.bfloat16),
        in_specs=[SMEM, VMEM, VMEM],
        out_specs=VMEM,
        compiler_params=pltpu.CompilerParams(**PARAMS),
    )(owners, probs, solved)


def solution(mesh):
    in_specs = (
        P(None, None, ("head", "seq"), None),
        P(None, "head", "seq", None),
        P(None, "head", "seq", None),
        P("head", None, None),
        P("head", None),
        P("head", None),
    )
    out_specs = P("head", "seq", None, None)
    return jax.shard_map(
        on_device, mesh=mesh, in_specs=in_specs, out_specs=out_specs, check_vma=False
    )
```

```python
import jax
import jax.numpy as jnp
from jax import lax
from jax.experimental import pallas as pl
from jax.experimental.pallas import tpu as pltpu
from jax.sharding import PartitionSpec as P

FITS_LAYER = 4
SLOTS = 3
RIDGE = 0.3
LANES = 128
FAR = -(2.0**100)
LOG2E = 1.4426950408889634
PAIR = 2

SUBLANES = 8
MESH = pl.DeviceIdType.MESH
NT = (((1,), (1,)), ((), ()))
TN = (((0,), (0,)), ((), ()))


def solve_rows(system, target, halfway):
    rows = system.shape[0]
    row = lax.broadcasted_iota(jnp.int32, (rows, 1), 0)
    if rows <= 64:
        for k in range(rows):
            if k == rows // 2:
                halfway()
            inverse = 1.0 / system[k : k + 1, k : k + 1]
            pivot_s = system[k : k + 1, :] * inverse
            pivot_t = target[k : k + 1, :] * inverse
            column = jnp.where(row == k, system[:, k : k + 1] - 1.0, system[:, k : k + 1])
            system = system - column * pivot_s
            target = target - column * pivot_t
        return target
    halfway()
    lane = lax.broadcasted_iota(jnp.int32, (1, rows), 1)

    def step(k, state):
        system, target = state
        column = jnp.sum(jnp.where(lane == k, system, 0.0), axis=1, keepdims=True)
        here = row == k
        inverse = 1.0 / jnp.sum(jnp.where(here, column, 0.0), axis=0, keepdims=True)
        pivot_s = jnp.sum(jnp.where(here, system, 0.0), axis=0, keepdims=True) * inverse
        pivot_t = jnp.sum(jnp.where(here, target, 0.0), axis=0, keepdims=True) * inverse
        column = jnp.where(here, column - 1.0, column)
        return system - column * pivot_s, target - column * pivot_t

    return lax.fori_loop(0, rows, step, (system, target))[1]


def split_exponent(block, capacity):
    tail = block[:, capacity:].astype(jnp.float32)
    return block[:, :capacity].astype(jnp.float32), tail[:, 0:1] + tail[:, 64:65]


def joined_exponent(expo, top, lane):
    high = top.astype(jnp.bfloat16)
    low = (top - high.astype(jnp.float32)).astype(jnp.bfloat16)
    tail = jnp.where(lane < 64, high.astype(jnp.float32), low.astype(jnp.float32))
    return jnp.concatenate([expo.astype(jnp.bfloat16), tail.astype(jnp.bfloat16)], axis=1)


def enter(axes):
    barrier = pltpu.get_barrier_semaphore()
    total = 0
    for axis in axes:
        me, size = lax.axis_index(axis), lax.axis_size(axis)
        for step in range(1, size):
            pl.semaphore_signal(
                barrier, inc=1, device_id={axis: lax.rem(me + step, size)}, device_id_type=MESH
            )
        total += size - 1
    pl.semaphore_wait(barrier, total)


def send(source, target, send_sem, recv_sem, axis, peer):
    return pltpu.make_async_remote_copy(
        src_ref=source,
        dst_ref=target,
        send_sem=send_sem,
        recv_sem=recv_sem,
        device_id={axis: peer},
        device_id_type=MESH,
    )


def query_kernel(q_ref, out_ref, piece, column, table, send_head, recv_head, send_seq, recv_seq):
    layers, heads, count, width = q_ref.shape
    my_head, my_seq = lax.axis_index("head"), lax.axis_index("seq")
    groups = lax.axis_size("seq")
    for head in range(heads):
        for layer in range(layers):
            piece[head, layer : layer + 1, :] = q_ref[layer, head].astype(jnp.float32)
        piece[head, layers:, :] = jnp.zeros((SUBLANES - layers, width), jnp.float32)
    enter(("head", "seq"))
    column[0] = piece[my_head]
    copies = []
    for step in range(1, heads):
        peer = lax.rem(my_head + step, heads)
        copies.append(
            send(
                piece.at[peer],
                column.at[step],
                send_head.at[step],
                recv_head.at[step],
                "head",
                peer,
            )
        )
        copies[-1].start()
    for copy in copies:
        copy.wait_recv()
    later = []
    for step in range(1, groups):
        peer = lax.rem(my_seq + step, groups)
        later.append(
            send(column, table.at[my_seq], send_seq.at[step], recv_seq.at[step], "seq", peer)
        )
        later[-1].start()
    table[my_seq] = column[...]
    for copy in copies:
        copy.wait_send()
    for copy in later:
        copy.wait()
    out_ref[...] = table[...]


def fit_kernel(
    sizes_ref, q_ref, k_ref, v_ref, idx_ref, p_ref, x_ref,
    s_ref, g_ref, part, part_in, chunk_mine, chunks, e_out, e_in, z_out, z_in,
    p_mine, p_all, x_mine, x_all,
    send_part, recv_part, send_chunk, recv_chunk, send_e, recv_e, send_z, recv_z,
    send_p, recv_p, send_f, recv_f, send_x, recv_x,
):
    layers, local_len, width = k_ref.shape
    rows = q_ref.shape[0] // SUBLANES
    fits, capacity = idx_ref.shape
    groups, me = lax.axis_size("seq"), lax.axis_index("seq")
    outer, inner = me // PAIR, lax.rem(me, PAIR)
    outers, half = groups // PAIR, fits // PAIR
    partner = outer * PAIR + 1 - inner
    fit_mine = jnp.minimum(me, fits - 1)
    chunk = layers * rows // groups
    start = me * local_len
    lane = lax.broadcasted_iota(jnp.int32, (rows, LANES), 1)
    exact = outers == half

    for layer in range(layers):
        query_rows = q_ref[pl.ds(layer, rows, stride=SUBLANES), :].astype(jnp.bfloat16)
        scores = lax.dot_general(
            query_rows, k_ref[layer], NT, preferred_element_type=jnp.float32
        ) * (width ** (-0.5) * LOG2E)
        s_ref[layer] = scores
        peak = jnp.max(scores, axis=1, keepdims=True)
        weights = jnp.exp2(scores - peak)
        total = jnp.sum(weights, axis=1, keepdims=True)
        numer = jnp.dot(
            weights.astype(jnp.bfloat16), v_ref[layer], preferred_element_type=jnp.float32
        )
        side = jnp.where(lane < 64, total, peak)
        for piece in range(rows // chunk):
            slot = layer * (rows // chunk) + piece
            part[slot, 0] = numer[piece * chunk : (piece + 1) * chunk]
            part[slot, 1] = side[piece * chunk : (piece + 1) * chunk]

    def produce(fit):
        layer = fit // FITS_LAYER
        size = sizes_ref[0, fit]

        def one_tile(tile, top):
            base = pl.multiple_of(tile * LANES, LANES)
            drawn = idx_ref[:, pl.ds(base, LANES)]
            mine = lax.broadcasted_iota(jnp.int32, (fits, LANES), 0) == fit
            offset = jnp.sum(jnp.where(mine, drawn, 0), axis=0, keepdims=True) - start
            column = base + lax.broadcasted_iota(jnp.int32, (1, LANES), 1)
            inside = (offset >= 0) & (offset < local_len) & (column < size)
            offset = jnp.broadcast_to(jnp.where(inside, offset, -1), (rows, LANES))
            high = offset >> 7
            low = offset & (LANES - 1)
            picked = jnp.full((rows, LANES), FAR, jnp.float32)
            for block in range(local_len // LANES):
                piece = s_ref[layer, :, block * LANES : (block + 1) * LANES]
                found = jnp.take_along_axis(piece, low, axis=1, mode="promise_in_bounds")
                picked = jnp.where(high == block, found, picked)
            g_ref[:, pl.ds(base, LANES)] = picked
            return jnp.maximum(top, jnp.max(picked, axis=1, keepdims=True))

        top = lax.fori_loop(
            0, capacity // LANES, one_tile, jnp.full((rows, 1), FAR, jnp.float32)
        )
        top = jnp.ceil(top)
        picked = g_ref[...]
        return jnp.where(picked > 0.5 * FAR, jnp.exp2(picked - top), 0.0), top

    enter(("seq",))
    parts = []
    for step in range(1, groups):
        peer = lax.rem(me + step, groups)
        parts.append(
            send(
                part.at[peer], part_in.at[step],
                send_part.at[step], recv_part.at[step], "seq", peer,
            )
        )
        parts[-1].start()
    part_in[0] = part[me]

    def column_of(j):
        return lax.rem(outer + 1 + j, outers) if exact else jnp.int32(j)

    across = []
    for j in range(half):
        expo, top = produce(column_of(j) * PAIR + 1 - inner)
        e_out[j] = joined_exponent(expo, top, lane)
        across.append(
            send(e_out.at[j], e_in.at[j], send_e.at[j], recv_e.at[j], "seq", partner)
        )
        if j > 0:
            across[j - 1].start()

    for copy in parts:
        copy.wait_recv()
    peak = part_in[0, 1][:, 64:65]
    for step in range(1, groups):
        peak = jnp.maximum(peak, part_in[step, 1][:, 64:65])
    numer, total = 0.0, 0.0
    for step in range(groups):
        factor = jnp.exp2(part_in[step, 1][:, 64:65] - peak)
        numer = numer + part_in[step, 0] * factor
        total = total + part_in[step, 1][:, 0:1] * factor
    merged = numer / total
    chunk_mine[...] = merged
    chunks[me] = merged
    across[half - 1].start()

    down, spread = [], []
    for j in range(half):
        dest = column_of(j)
        expo, top = produce(dest * PAIR + inner)
        if j == 0:
            for step in range(1, groups):
                peer = lax.rem(me + step, groups)
                spread.append(
                    send(
                        chunk_mine, chunks.at[me],
                        send_chunk.at[step], recv_chunk.at[step], "seq", peer,
                    )
                )
                spread[-1].start()
        across[j].wait_recv()
        other, other_top = split_exponent(e_in[j], capacity)
        both = jnp.maximum(top, other_top)
        expo = expo * jnp.exp2(top - both) + other * jnp.exp2(other_top - both)
        block = joined_exponent(expo, both, lane)
        copy = send(
            z_out.at[j], z_in.at[outer], send_z.at[j], recv_z.at[outer],
            "seq", dest * PAIR + inner,
        )
        down.append((dest, copy))
        if exact:
            if j == half - 1:
                z_in[outer] = block
            else:
                z_out[j] = block
                copy.start()
        else:
            z_out[j] = block
            pl.when(dest != outer)(copy.start)

            @pl.when(dest == outer)
            def _():
                z_in[outer] = block

    def only(condition, act):
        if exact:
            act()
        else:
            pl.when(condition)(act)

    def source_z(step):
        source = lax.rem(outer + step, outers)
        return source, send(
            z_out.at[0], z_in.at[source], send_z.at[0], recv_z.at[source], "seq", partner
        )

    def gave_p(step, target):
        return send(
            p_mine, p_all.at[fit_mine], send_p.at[step], recv_p.at[outer],
            "seq", target * PAIR + inner,
        )

    def came_p(source):
        fit = jnp.minimum(source, half - 1) * PAIR + inner
        arrival = send(
            p_mine, p_all.at[fit], send_p.at[0], recv_p.at[source], "seq", partner
        )
        onward = send(
            p_all.at[fit], p_all.at[fit], send_f.at[source], recv_f.at[source], "seq", partner
        )
        return arrival, onward

    def back_p(source):
        fit = jnp.minimum(source, half - 1) * PAIR + 1 - inner
        return send(
            p_mine, p_all.at[fit], send_f.at[source], recv_f.at[source], "seq", partner
        )

    gifts = [gave_p(step, lax.rem(outer + step, outers)) for step in range(1, outers)]
    own_onward = send(
        p_mine, p_all.at[fit_mine], send_f.at[outer], recv_f.at[outer], "seq", partner
    )
    results = [
        send(
            x_mine, x_all.at[fit_mine], send_x.at[step], recv_x.at[step],
            "seq", lax.rem(me + step, groups),
        )
        for step in range(1, groups)
    ]

    def relay():
        for step in range(1, outers):
            source = lax.rem(outer + outers - step, outers)
            arrival, onward = came_p(source)

            def pass_on():
                arrival.wait_recv()
                onward.start()

            only(source < half, pass_on)

    for copy in spread:
        copy.wait_recv()

    def work():
        for step in range(1, outers):
            source_z(step)[1].wait_recv()
        blocks = [split_exponent(z_in[source], capacity) for source in range(outers)]
        top = blocks[0][1]
        for _, other in blocks[1:]:
            top = jnp.maximum(top, other)
        probs = 0.0
        for expo, other in blocks:
            probs = probs + expo * jnp.exp2(other - top)
        probs = (probs / jnp.sum(probs, axis=1, keepdims=True)).astype(jnp.bfloat16)
        p_mine[...] = probs
        p_all[fit_mine] = probs
        gram = lax.dot_general(probs, probs, NT, preferred_element_type=jnp.float32)
        for copy in gifts:
            copy.start()
        own_onward.start()
        diagonal = lax.broadcasted_iota(jnp.int32, (rows, rows), 0) == lax.broadcasted_iota(
            jnp.int32, (rows, rows), 1
        )
        trace = jnp.sum(jnp.where(diagonal, gram, 0.0))
        ridge = RIDGE * trace / sizes_ref[0, fit_mine].astype(jnp.float32)
        span = rows // chunk
        first = (fit_mine // FITS_LAYER) * span
        target = jnp.concatenate([chunks[first + piece] for piece in range(span)], axis=0)
        target = target.astype(jnp.bfloat16).astype(jnp.float32)
        solved = solve_rows(
            jnp.where(diagonal, gram + ridge, gram), target, relay if exact else lambda: None
        )
        x_mine[...] = solved
        x_all[fit_mine] = solved
        for copy in results:
            copy.start()

    only(outer < half, work)
    if not exact:
        relay()
    for copy in parts + spread + across:
        copy.wait_send()
    for j in range(half):
        dest, copy = down[j]
        if exact:
            if j < half - 1:
                copy.wait_send()
        else:
            pl.when(dest != outer)(copy.wait_send)
    for step in range(1, outers):
        source = lax.rem(outer + outers - step, outers)
        only(outer < half, gifts[step - 1].wait_send)
        only(source < half, came_p(source)[1].wait_send)
    only(outer < half, own_onward.wait_send)
    for source in range(half):
        back_p(source).wait_recv()
    for step in range(1, groups):
        source = lax.rem(me + groups - step, groups)
        only(source < fits, results[step - 1].wait_recv)
        only(outer < half, results[step - 1].wait_send)
    p_ref[...] = p_all[...]
    x_ref[...] = x_all[...]


def place_kernel(owners_ref, p_ref, x_ref, out_ref):
    me = lax.axis_index("seq")
    fits = p_ref.shape[0]
    count = jnp.int32(0)
    chosen = [jnp.int32(0)] * SLOTS
    for fit in range(fits):
        mine = owners_ref[0, fit] == me
        for slot in range(SLOTS):
            chosen[slot] = jnp.where(mine & (count == slot), fit, chosen[slot])
        count = count + mine.astype(jnp.int32)
    for slot in range(SLOTS):

        @pl.when(count > slot)
        def _():
            probs = p_ref[chosen[slot]]
            rows = x_ref[chosen[slot]]
            high = rows.astype(jnp.bfloat16)
            low = (rows - high.astype(jnp.float32)).astype(jnp.bfloat16)
            out_ref[0, slot] = lax.dot_general(
                jnp.concatenate([probs, probs], axis=0),
                jnp.concatenate([high, low], axis=0),
                TN,
                preferred_element_type=jnp.float32,
            ).astype(jnp.bfloat16)

        @pl.when(count <= slot)
        def _():
            out_ref[0, slot] = jnp.zeros(out_ref.shape[2:], jnp.bfloat16)


VMEM = pl.BlockSpec(memory_space=pltpu.VMEM)
SMEM = pl.BlockSpec(memory_space=pltpu.SMEM)
PARAMS = dict(vmem_limit_bytes=60 * 1024 * 1024)


def on_device(queries, keys, values, indices, sizes, owners):
    layers, heads, count, width = queries.shape
    groups = lax.axis_size("seq")
    rows = groups * heads * count
    local_len = keys.shape[2]
    fits, capacity = indices.shape[1:]
    dma = pltpu.SemaphoreType.DMA
    all_queries = pl.pallas_call(
        query_kernel,
        out_shape=jax.ShapeDtypeStruct((groups, heads, SUBLANES, width), jnp.float32),
        in_specs=[VMEM],
        out_specs=VMEM,
        scratch_shapes=[
            pltpu.VMEM((heads, SUBLANES, width), jnp.float32),
            pltpu.VMEM((heads, SUBLANES, width), jnp.float32),
            pltpu.VMEM((groups, heads, SUBLANES, width), jnp.float32),
            dma((heads,)),
            dma((heads,)),
            dma((groups,)),
            dma((groups,)),
        ],
        compiler_params=pltpu.CompilerParams(collective_id=1, has_side_effects=True, **PARAMS),
    )(queries)
    outers, half = groups // PAIR, fits // PAIR
    chunk = layers * rows // groups
    packed = (rows, capacity + LANES)
    probs, solved = pl.pallas_call(
        fit_kernel,
        out_shape=(
            jax.ShapeDtypeStruct((fits, rows, capacity), jnp.bfloat16),
            jax.ShapeDtypeStruct((fits, rows, width), jnp.float32),
        ),
        in_specs=[SMEM] + [VMEM] * 4,
        out_specs=(VMEM, VMEM),
        scratch_shapes=[
            pltpu.VMEM((layers, rows, local_len), jnp.float32),
            pltpu.VMEM((rows, capacity), jnp.float32),
            pltpu.VMEM((groups, 2, chunk, width), jnp.float32),
            pltpu.VMEM((groups, 2, chunk, width), jnp.float32),
            pltpu.VMEM((chunk, width), jnp.float32),
            pltpu.VMEM((groups, chunk, width), jnp.float32),
            pltpu.VMEM((half,) + packed, jnp.bfloat16),
            pltpu.VMEM((half,) + packed, jnp.bfloat16),
            pltpu.VMEM((half,) + packed, jnp.bfloat16),
            pltpu.VMEM((outers,) + packed, jnp.bfloat16),
            pltpu.VMEM((rows, capacity), jnp.bfloat16),
            pltpu.VMEM((fits, rows, capacity), jnp.bfloat16),
            pltpu.VMEM((rows, width), jnp.float32),
            pltpu.VMEM((fits, rows, width), jnp.float32),
            dma((groups,)),
            dma((groups,)),
            dma((groups,)),
            dma((groups,)),
            dma((half,)),
            dma((half,)),
            dma((half,)),
            dma((outers,)),
            dma((outers,)),
            dma((outers,)),
            dma((outers,)),
            dma((outers,)),
            dma((groups,)),
            dma((groups,)),
        ],
        compiler_params=pltpu.CompilerParams(collective_id=2, has_side_effects=True, **PARAMS),
    )(
        sizes,
        all_queries.reshape(rows * SUBLANES, width),
        keys[:, 0],
        values[:, 0],
        indices[0],
    )
    return pl.pallas_call(
        place_kernel,
        out_shape=jax.ShapeDtypeStruct((1, SLOTS, capacity, width), jnp.bfloat16),
        in_specs=[SMEM, VMEM, VMEM],
        out_specs=VMEM,
        compiler_params=pltpu.CompilerParams(**PARAMS),
    )(owners, probs, solved)


def solution(mesh):
    in_specs = (
        P(None, None, ("head", "seq"), None),
        P(None, "head", "seq", None),
        P(None, "head", "seq", None),
        P("head", None, None),
        P("head", None),
        P("head", None),
    )
    out_specs = P("head", "seq", None, None)
    return jax.shard_map(
        on_device, mesh=mesh, in_specs=in_specs, out_specs=out_specs, check_vma=False
    )
```

```python
import jax
import jax.numpy as jnp
from jax import lax
from jax.experimental import pallas as pl
from jax.experimental.pallas import tpu as pltpu
from jax.sharding import PartitionSpec as P

FITS_LAYER = 4
SLOTS = 3
RIDGE = 0.3
LANES = 128
FAR = -(2.0**100)
LOG2E = 1.4426950408889634
PAIR = 2

SUBLANES = 8
MESH = pl.DeviceIdType.MESH
NT = (((1,), (1,)), ((), ()))
TN = (((0,), (0,)), ((), ()))


def solve_rows(system, target):
    rows = system.shape[0]
    row = lax.broadcasted_iota(jnp.int32, (rows, 1), 0)
    if rows <= 64:
        for k in range(rows):
            inverse = 1.0 / system[k : k + 1, k : k + 1]
            pivot_s = system[k : k + 1, :] * inverse
            pivot_t = target[k : k + 1, :] * inverse
            column = jnp.where(row == k, system[:, k : k + 1] - 1.0, system[:, k : k + 1])
            system = system - column * pivot_s
            target = target - column * pivot_t
        return target
    lane = lax.broadcasted_iota(jnp.int32, (1, rows), 1)

    def step(k, state):
        system, target = state
        column = jnp.sum(jnp.where(lane == k, system, 0.0), axis=1, keepdims=True)
        here = row == k
        inverse = 1.0 / jnp.sum(jnp.where(here, column, 0.0), axis=0, keepdims=True)
        pivot_s = jnp.sum(jnp.where(here, system, 0.0), axis=0, keepdims=True) * inverse
        pivot_t = jnp.sum(jnp.where(here, target, 0.0), axis=0, keepdims=True) * inverse
        column = jnp.where(here, column - 1.0, column)
        return system - column * pivot_s, target - column * pivot_t

    return lax.fori_loop(0, rows, step, (system, target))[1]


def split_exponent(block, capacity):
    tail = block[:, capacity:].astype(jnp.float32)
    return block[:, :capacity].astype(jnp.float32), tail[:, 0:1] + tail[:, 64:65]


def joined_exponent(expo, top, lane):
    high = top.astype(jnp.bfloat16)
    low = (top - high.astype(jnp.float32)).astype(jnp.bfloat16)
    tail = jnp.where(lane < 64, high.astype(jnp.float32), low.astype(jnp.float32))
    return jnp.concatenate([expo.astype(jnp.bfloat16), tail.astype(jnp.bfloat16)], axis=1)


def enter(axes):
    barrier = pltpu.get_barrier_semaphore()
    total = 0
    for axis in axes:
        me, size = lax.axis_index(axis), lax.axis_size(axis)
        for step in range(1, size):
            pl.semaphore_signal(
                barrier, inc=1, device_id={axis: lax.rem(me + step, size)}, device_id_type=MESH
            )
        total += size - 1
    pl.semaphore_wait(barrier, total)


def send(source, target, send_sem, recv_sem, axis, peer):
    return pltpu.make_async_remote_copy(
        src_ref=source,
        dst_ref=target,
        send_sem=send_sem,
        recv_sem=recv_sem,
        device_id={axis: peer},
        device_id_type=MESH,
    )


def fit_kernel(
    sizes_ref, q_in, k_hbm, v_hbm, idx_ref, p_ref, x_ref,
    piece, column, table, k_ref, v_ref, s_ref, g_ref, part, part_in, chunk_mine, chunks, e_out, e_in, z_out, z_in,
    p_mine, p_all, x_mine, x_all,
    load, send_head, recv_head, send_seq, recv_seq, send_part, recv_part, send_chunk, recv_chunk, send_e, recv_e, send_z, recv_z,
    send_p, recv_p, send_f, recv_f, send_x, recv_x,
):
    layers, local_len, width = k_ref.shape
    fits, capacity = idx_ref.shape
    heads, my_head = lax.axis_size("head"), lax.axis_index("head")
    groups, me = lax.axis_size("seq"), lax.axis_index("seq")
    rows = groups * heads
    outer, inner = me // PAIR, lax.rem(me, PAIR)
    outers, half = groups // PAIR, fits // PAIR
    partner = outer * PAIR + 1 - inner
    fit_mine = jnp.minimum(me, fits - 1)
    chunk = layers * rows // groups
    start = me * local_len
    lane = lax.broadcasted_iota(jnp.int32, (rows, LANES), 1)
    exact = outers == half

    loads = [
        pltpu.make_async_copy(k_hbm, k_ref, load.at[0]),
        pltpu.make_async_copy(v_hbm, v_ref, load.at[1]),
    ]
    for copy in loads:
        copy.start()
    drawn_rows = q_in[...].astype(jnp.float32)
    for head in range(heads):
        for layer in range(layers):
            at = layer * heads + head
            piece[head, layer : layer + 1, :] = drawn_rows[at : at + 1]
        piece[head, layers:, :] = jnp.zeros((SUBLANES - layers, width), jnp.float32)
    enter(("head", "seq"))
    near = heads * SUBLANES
    column[pl.ds(pl.multiple_of(my_head * SUBLANES, SUBLANES), SUBLANES), :] = piece[my_head]
    first, second = [], []
    for step in range(1, heads):
        peer = lax.rem(my_head + step, heads)
        first.append(
            send(
                piece.at[peer],
                column.at[pl.ds(pl.multiple_of(my_head * SUBLANES, SUBLANES), SUBLANES), :],
                send_head.at[step], recv_head.at[step], "head", peer,
            )
        )
        first[-1].start()
    for copy in first:
        copy.wait_recv()
    for step in range(1, groups):
        peer = lax.rem(me + step, groups)
        second.append(
            send(
                column, table.at[pl.ds(pl.multiple_of(me * near, near), near), :],
                send_seq.at[step], recv_seq.at[step], "seq", peer,
            )
        )
        second[-1].start()
    table[pl.ds(pl.multiple_of(me * near, near), near), :] = column[...]
    for copy in second:
        copy.wait_recv()
    for copy in loads:
        copy.wait()

    for layer in range(layers):
        query_rows = table[pl.ds(layer, rows, stride=SUBLANES), :].astype(jnp.bfloat16)
        scores = lax.dot_general(
            query_rows, k_ref[layer], NT, preferred_element_type=jnp.float32
        ) * (width ** (-0.5) * LOG2E)
        s_ref[layer] = scores
        peak = jnp.max(scores, axis=1, keepdims=True)
        weights = jnp.exp2(scores - peak)
        total = jnp.sum(weights, axis=1, keepdims=True)
        numer = jnp.dot(
            weights.astype(jnp.bfloat16), v_ref[layer], preferred_element_type=jnp.float32
        )
        side = jnp.where(lane < 64, total, peak)
        for at in range(rows // chunk):
            slot = layer * (rows // chunk) + at
            part[slot, 0] = numer[at * chunk : (at + 1) * chunk]
            part[slot, 1] = side[at * chunk : (at + 1) * chunk]

    def produce(fit):
        layer = fit // FITS_LAYER
        size = sizes_ref[0, fit]

        def one_tile(tile, top):
            base = pl.multiple_of(tile * LANES, LANES)
            drawn = idx_ref[:, pl.ds(base, LANES)]
            mine = lax.broadcasted_iota(jnp.int32, (fits, LANES), 0) == fit
            offset = jnp.sum(jnp.where(mine, drawn, 0), axis=0, keepdims=True) - start
            column = base + lax.broadcasted_iota(jnp.int32, (1, LANES), 1)
            inside = (offset >= 0) & (offset < local_len) & (column < size)
            offset = jnp.broadcast_to(jnp.where(inside, offset, -1), (rows, LANES))
            high = offset >> 7
            low = offset & (LANES - 1)
            picked = jnp.full((rows, LANES), FAR, jnp.float32)
            for block in range(local_len // LANES):
                scored = s_ref[layer, :, block * LANES : (block + 1) * LANES]
                found = jnp.take_along_axis(scored, low, axis=1, mode="promise_in_bounds")
                picked = jnp.where(high == block, found, picked)
            g_ref[:, pl.ds(base, LANES)] = picked
            return jnp.maximum(top, jnp.max(picked, axis=1, keepdims=True))

        top = lax.fori_loop(
            0,
            capacity // LANES,
            one_tile,
            jnp.full((rows, 1), FAR, jnp.float32),
            unroll=4 if rows <= 64 else 1,
        )
        top = jnp.ceil(top)
        picked = g_ref[...]
        return jnp.where(picked > 0.5 * FAR, jnp.exp2(picked - top), 0.0), top

    parts = []
    for step in range(1, groups):
        peer = lax.rem(me + step, groups)
        parts.append(
            send(
                part.at[peer], part_in.at[step],
                send_part.at[step], recv_part.at[step], "seq", peer,
            )
        )
        parts[-1].start()
    part_in[0] = part[me]

    def column_of(j):
        return lax.rem(outer + 1 + j, outers) if exact else jnp.int32(j)

    across = []
    for j in range(half):
        expo, top = produce(column_of(j) * PAIR + 1 - inner)
        e_out[j] = joined_exponent(expo, top, lane)
        across.append(
            send(e_out.at[j], e_in.at[j], send_e.at[j], recv_e.at[j], "seq", partner)
        )
        if j > 0:
            across[j - 1].start()

    for copy in parts:
        copy.wait_recv()
    peak = part_in[0, 1][:, 64:65]
    for step in range(1, groups):
        peak = jnp.maximum(peak, part_in[step, 1][:, 64:65])
    numer, total = 0.0, 0.0
    for step in range(groups):
        factor = jnp.exp2(part_in[step, 1][:, 64:65] - peak)
        numer = numer + part_in[step, 0] * factor
        total = total + part_in[step, 1][:, 0:1] * factor
    merged = numer / total
    chunk_mine[...] = merged
    chunks[me] = merged
    across[half - 1].start()

    down, spread = [], []
    for j in range(half):
        dest = column_of(j)
        expo, top = produce(dest * PAIR + inner)
        if j == 0:
            for step in range(1, groups):
                peer = lax.rem(me + step, groups)
                spread.append(
                    send(
                        chunk_mine, chunks.at[me],
                        send_chunk.at[step], recv_chunk.at[step], "seq", peer,
                    )
                )
                spread[-1].start()
        across[j].wait_recv()
        other, other_top = split_exponent(e_in[j], capacity)
        both = jnp.maximum(top, other_top)
        expo = expo * jnp.exp2(top - both) + other * jnp.exp2(other_top - both)
        block = joined_exponent(expo, both, lane)
        copy = send(
            z_out.at[j], z_in.at[outer], send_z.at[j], recv_z.at[outer],
            "seq", dest * PAIR + inner,
        )
        down.append((dest, copy))
        if exact:
            if j == half - 1:
                z_in[outer] = block
            else:
                z_out[j] = block
                copy.start()
        else:
            z_out[j] = block
            pl.when(dest != outer)(copy.start)

            @pl.when(dest == outer)
            def _():
                z_in[outer] = block

    def only(condition, act):
        if exact:
            act()
        else:
            pl.when(condition)(act)

    def source_z(step):
        source = lax.rem(outer + step, outers)
        return source, send(
            z_out.at[0], z_in.at[source], send_z.at[0], recv_z.at[source], "seq", partner
        )

    def gave_p(step, target):
        return send(
            p_mine, p_all.at[fit_mine], send_p.at[step], recv_p.at[outer],
            "seq", target * PAIR + inner,
        )

    def came_p(source):
        fit = jnp.minimum(source, half - 1) * PAIR + inner
        arrival = send(
            p_mine, p_all.at[fit], send_p.at[0], recv_p.at[source], "seq", partner
        )
        onward = send(
            p_all.at[fit], p_all.at[fit], send_f.at[source], recv_f.at[source], "seq", partner
        )
        return arrival, onward

    def back_p(source):
        fit = jnp.minimum(source, half - 1) * PAIR + 1 - inner
        return send(
            p_mine, p_all.at[fit], send_f.at[source], recv_f.at[source], "seq", partner
        )

    gifts = [gave_p(step, lax.rem(outer + step, outers)) for step in range(1, outers)]
    own_onward = send(
        p_mine, p_all.at[fit_mine], send_f.at[outer], recv_f.at[outer], "seq", partner
    )
    results = [
        send(
            x_mine, x_all.at[fit_mine], send_x.at[step], recv_x.at[step],
            "seq", lax.rem(me + step, groups),
        )
        for step in range(1, groups)
    ]

    def relay():
        for step in range(1, outers):
            source = lax.rem(outer + outers - step, outers)
            arrival, onward = came_p(source)

            def pass_on():
                arrival.wait_recv()
                onward.start()

            only(source < half, pass_on)

    for copy in spread:
        copy.wait_recv()

    def work():
        for step in range(1, outers):
            source_z(step)[1].wait_recv()
        blocks = [split_exponent(z_in[source], capacity) for source in range(outers)]
        top = blocks[0][1]
        for _, other in blocks[1:]:
            top = jnp.maximum(top, other)
        probs = 0.0
        for expo, other in blocks:
            probs = probs + expo * jnp.exp2(other - top)
        probs = (probs / jnp.sum(probs, axis=1, keepdims=True)).astype(jnp.bfloat16)
        p_mine[...] = probs
        p_all[fit_mine] = probs
        gram = lax.dot_general(probs, probs, NT, preferred_element_type=jnp.float32)
        for copy in gifts:
            copy.start()
        own_onward.start()
        diagonal = lax.broadcasted_iota(jnp.int32, (rows, rows), 0) == lax.broadcasted_iota(
            jnp.int32, (rows, rows), 1
        )
        trace = jnp.sum(jnp.where(diagonal, gram, 0.0))
        ridge = RIDGE * trace / sizes_ref[0, fit_mine].astype(jnp.float32)
        span = rows // chunk
        base = (fit_mine // FITS_LAYER) * span
        target = jnp.concatenate([chunks[base + at] for at in range(span)], axis=0)
        target = target.astype(jnp.bfloat16).astype(jnp.float32)
        solved = solve_rows(jnp.where(diagonal, gram + ridge, gram), target)
        x_mine[...] = solved
        x_all[fit_mine] = solved
        for copy in results:
            copy.start()

    only(outer < half, work)
    relay()
    for copy in first + second + parts + spread + across:
        copy.wait_send()
    for j in range(half):
        dest, copy = down[j]
        if exact:
            if j < half - 1:
                copy.wait_send()
        else:
            pl.when(dest != outer)(copy.wait_send)
    for step in range(1, outers):
        source = lax.rem(outer + outers - step, outers)
        only(outer < half, gifts[step - 1].wait_send)
        only(source < half, came_p(source)[1].wait_send)
    only(outer < half, own_onward.wait_send)
    for source in range(half):
        back_p(source).wait_recv()
    for step in range(1, groups):
        source = lax.rem(me + groups - step, groups)
        only(source < fits, results[step - 1].wait_recv)
        only(outer < half, results[step - 1].wait_send)
    p_ref[...] = p_all[...]
    x_ref[...] = x_all[...]


def place_kernel(owners_ref, p_ref, x_ref, out_ref):
    me = lax.axis_index("seq")
    fits = p_ref.shape[0]
    count = jnp.int32(0)
    chosen = [jnp.int32(0)] * SLOTS
    for fit in range(fits):
        mine = owners_ref[0, fit] == me
        for slot in range(SLOTS):
            chosen[slot] = jnp.where(mine & (count == slot), fit, chosen[slot])
        count = count + mine.astype(jnp.int32)
    for slot in range(SLOTS):

        @pl.when(count > slot)
        def _():
            probs = p_ref[chosen[slot]]
            rows = x_ref[chosen[slot]]
            high = rows.astype(jnp.bfloat16)
            low = (rows - high.astype(jnp.float32)).astype(jnp.bfloat16)
            out_ref[0, slot] = lax.dot_general(
                jnp.concatenate([probs, probs], axis=0),
                jnp.concatenate([high, low], axis=0),
                TN,
                preferred_element_type=jnp.float32,
            ).astype(jnp.bfloat16)

        @pl.when(count <= slot)
        def _():
            out_ref[0, slot] = jnp.zeros(out_ref.shape[2:], jnp.bfloat16)


VMEM = pl.BlockSpec(memory_space=pltpu.VMEM)
ANY = pl.BlockSpec(memory_space=pl.ANY)
SMEM = pl.BlockSpec(memory_space=pltpu.SMEM)
PARAMS = dict(vmem_limit_bytes=60 * 1024 * 1024)


def on_device(queries, keys, values, indices, sizes, owners):
    layers, heads, count, width = queries.shape
    groups = lax.axis_size("seq")
    rows = groups * heads * count
    local_len = keys.shape[2]
    fits, capacity = indices.shape[1:]
    dma = pltpu.SemaphoreType.DMA
    outers, half = groups // PAIR, fits // PAIR
    chunk = layers * rows // groups
    packed = (rows, capacity + LANES)
    probs, solved = pl.pallas_call(
        fit_kernel,
        out_shape=(
            jax.ShapeDtypeStruct((fits, rows, capacity), jnp.bfloat16),
            jax.ShapeDtypeStruct((fits, rows, width), jnp.float32),
        ),
        in_specs=[SMEM, VMEM, ANY, ANY, VMEM],
        out_specs=(VMEM, VMEM),
        scratch_shapes=[
            pltpu.VMEM((heads, SUBLANES, width), jnp.float32),
            pltpu.VMEM((heads * SUBLANES, width), jnp.float32),
            pltpu.VMEM((rows * SUBLANES, width), jnp.float32),
            pltpu.VMEM((layers, local_len, width), jnp.bfloat16),
            pltpu.VMEM((layers, local_len, width), jnp.bfloat16),
            pltpu.VMEM((layers, rows, local_len), jnp.float32),
            pltpu.VMEM((rows, capacity), jnp.float32),
            pltpu.VMEM((groups, 2, chunk, width), jnp.float32),
            pltpu.VMEM((groups, 2, chunk, width), jnp.float32),
            pltpu.VMEM((chunk, width), jnp.float32),
            pltpu.VMEM((groups, chunk, width), jnp.float32),
            pltpu.VMEM((half,) + packed, jnp.bfloat16),
            pltpu.VMEM((half,) + packed, jnp.bfloat16),
            pltpu.VMEM((half,) + packed, jnp.bfloat16),
            pltpu.VMEM((outers,) + packed, jnp.bfloat16),
            pltpu.VMEM((rows, capacity), jnp.bfloat16),
            pltpu.VMEM((fits, rows, capacity), jnp.bfloat16),
            pltpu.VMEM((rows, width), jnp.float32),
            pltpu.VMEM((fits, rows, width), jnp.float32),
            dma((2,)),
            dma((heads,)),
            dma((heads,)),
            dma((groups,)),
            dma((groups,)),
            dma((groups,)),
            dma((groups,)),
            dma((groups,)),
            dma((groups,)),
            dma((half,)),
            dma((half,)),
            dma((half,)),
            dma((outers,)),
            dma((outers,)),
            dma((outers,)),
            dma((outers,)),
            dma((outers,)),
            dma((groups,)),
            dma((groups,)),
        ],
        compiler_params=pltpu.CompilerParams(collective_id=2, has_side_effects=True, **PARAMS),
    )(
        sizes,
        queries.reshape(layers * heads, width),
        keys[:, 0],
        values[:, 0],
        indices[0],
    )
    return pl.pallas_call(
        place_kernel,
        out_shape=jax.ShapeDtypeStruct((1, SLOTS, capacity, width), jnp.bfloat16),
        in_specs=[SMEM, VMEM, VMEM],
        out_specs=VMEM,
        compiler_params=pltpu.CompilerParams(**PARAMS),
    )(owners, probs, solved)


def solution(mesh):
    in_specs = (
        P(None, None, ("head", "seq"), None),
        P(None, "head", "seq", None),
        P(None, "head", "seq", None),
        P("head", None, None),
        P("head", None),
        P("head", None),
    )
    out_specs = P("head", "seq", None, None)
    return jax.shard_map(
        on_device, mesh=mesh, in_specs=in_specs, out_specs=out_specs, check_vma=False
    )
```

```python
import jax
import jax.numpy as jnp
from jax import lax
from jax.experimental import pallas as pl
from jax.experimental.pallas import tpu as pltpu
from jax.sharding import PartitionSpec as P

FITS_LAYER = 4
SLOTS = 3
RIDGE = 0.3
LANES = 128
FAR = -(2.0**100)
LOG2E = 1.4426950408889634
PAIR = 2

SUBLANES = 8
MESH = pl.DeviceIdType.MESH
NT = (((1,), (1,)), ((), ()))
TN = (((0,), (0,)), ((), ()))


def solve_rows(system, target):
    rows = system.shape[0]
    row = lax.broadcasted_iota(jnp.int32, (rows, 1), 0)
    if rows <= 64:
        for k in range(rows):
            inverse = 1.0 / system[k : k + 1, k : k + 1]
            pivot_s = system[k : k + 1, :] * inverse
            pivot_t = target[k : k + 1, :] * inverse
            column = jnp.where(row == k, system[:, k : k + 1] - 1.0, system[:, k : k + 1])
            system = system - column * pivot_s
            target = target - column * pivot_t
        return target
    lane = lax.broadcasted_iota(jnp.int32, (1, rows), 1)

    def step(k, state):
        system, target = state
        column = jnp.sum(jnp.where(lane == k, system, 0.0), axis=1, keepdims=True)
        here = row == k
        inverse = 1.0 / jnp.sum(jnp.where(here, column, 0.0), axis=0, keepdims=True)
        pivot_s = jnp.sum(jnp.where(here, system, 0.0), axis=0, keepdims=True) * inverse
        pivot_t = jnp.sum(jnp.where(here, target, 0.0), axis=0, keepdims=True) * inverse
        column = jnp.where(here, column - 1.0, column)
        return system - column * pivot_s, target - column * pivot_t

    return lax.fori_loop(0, rows, step, (system, target))[1]


def split_exponent(block, capacity):
    tail = block[:, capacity:].astype(jnp.float32)
    return block[:, :capacity].astype(jnp.float32), tail[:, 0:1] + tail[:, 64:65]


def joined_exponent(expo, top, lane):
    high = top.astype(jnp.bfloat16)
    low = (top - high.astype(jnp.float32)).astype(jnp.bfloat16)
    tail = jnp.where(lane < 64, high.astype(jnp.float32), low.astype(jnp.float32))
    return jnp.concatenate([expo.astype(jnp.bfloat16), tail.astype(jnp.bfloat16)], axis=1)


def enter(axes):
    barrier = pltpu.get_barrier_semaphore()
    total = 0
    for axis in axes:
        me, size = lax.axis_index(axis), lax.axis_size(axis)
        for step in range(1, size):
            pl.semaphore_signal(
                barrier, inc=1, device_id={axis: lax.rem(me + step, size)}, device_id_type=MESH
            )
        total += size - 1
    pl.semaphore_wait(barrier, total)


def send(source, target, send_sem, recv_sem, axis, peer):
    return pltpu.make_async_remote_copy(
        src_ref=source,
        dst_ref=target,
        send_sem=send_sem,
        recv_sem=recv_sem,
        device_id={axis: peer},
        device_id_type=MESH,
    )


def fit_kernel(
    sizes_ref, q_in, k_hbm, v_hbm, idx_ref, p_ref, x_ref,
    piece, column, table, k_ref, v_ref, s_ref, g_ref, part, part_in, chunk_mine, chunks, e_out, e_in, z_out, z_in,
    p_mine, p_all, x_mine, x_all,
    load, send_head, recv_head, send_seq, recv_seq, send_part, recv_part, send_chunk, recv_chunk, send_e, recv_e, send_z, recv_z,
    send_p, recv_p, send_f, recv_f, send_x, recv_x,
):
    layers, local_len, width = k_ref.shape
    fits, capacity = idx_ref.shape
    heads, my_head = lax.axis_size("head"), lax.axis_index("head")
    groups, me = lax.axis_size("seq"), lax.axis_index("seq")
    rows = groups * heads
    outer, inner = me // PAIR, lax.rem(me, PAIR)
    outers, half = groups // PAIR, fits // PAIR
    partner = outer * PAIR + 1 - inner
    fit_mine = jnp.minimum(me, fits - 1)
    chunk = layers * rows // groups
    start = me * local_len
    lane = lax.broadcasted_iota(jnp.int32, (rows, LANES), 1)
    exact = outers == half

    loads = [
        pltpu.make_async_copy(k_hbm, k_ref, load.at[0]),
        pltpu.make_async_copy(v_hbm, v_ref, load.at[1]),
    ]
    for copy in loads:
        copy.start()
    drawn_rows = q_in[...].astype(jnp.float32)
    for head in range(heads):
        for layer in range(layers):
            at = layer * heads + head
            piece[head, layer : layer + 1, :] = drawn_rows[at : at + 1]
        piece[head, layers:, :] = jnp.zeros((SUBLANES - layers, width), jnp.float32)
    enter(("head", "seq"))
    near = heads * SUBLANES
    column[pl.ds(pl.multiple_of(my_head * SUBLANES, SUBLANES), SUBLANES), :] = piece[my_head]
    first, second = [], []
    for step in range(1, heads):
        peer = lax.rem(my_head + step, heads)
        first.append(
            send(
                piece.at[peer],
                column.at[pl.ds(pl.multiple_of(my_head * SUBLANES, SUBLANES), SUBLANES), :],
                send_head.at[step], recv_head.at[step], "head", peer,
            )
        )
        first[-1].start()
    for copy in first:
        copy.wait_recv()
    for step in range(1, groups):
        peer = lax.rem(me + step, groups)
        second.append(
            send(
                column, table.at[pl.ds(pl.multiple_of(me * near, near), near), :],
                send_seq.at[step], recv_seq.at[step], "seq", peer,
            )
        )
        second[-1].start()
    table[pl.ds(pl.multiple_of(me * near, near), near), :] = column[...]
    for copy in second:
        copy.wait_recv()
    for copy in loads:
        copy.wait()

    for layer in range(layers):
        query_rows = table[pl.ds(layer, rows, stride=SUBLANES), :].astype(jnp.bfloat16)
        scores = lax.dot_general(
            query_rows, k_ref[layer], NT, preferred_element_type=jnp.float32
        ) * (width ** (-0.5) * LOG2E)
        s_ref[layer] = scores
        peak = jnp.max(scores, axis=1, keepdims=True)
        weights = jnp.exp2(scores - peak)
        total = jnp.sum(weights, axis=1, keepdims=True)
        numer = jnp.dot(
            weights.astype(jnp.bfloat16), v_ref[layer], preferred_element_type=jnp.float32
        )
        side = jnp.where(lane < 64, total, peak)
        for at in range(rows // chunk):
            slot = layer * (rows // chunk) + at
            part[slot, 0] = numer[at * chunk : (at + 1) * chunk]
            part[slot, 1] = side[at * chunk : (at + 1) * chunk]

    def produce(fit):
        layer = fit // FITS_LAYER
        size = sizes_ref[0, fit]

        def one_tile(tile, top):
            base = pl.multiple_of(tile * LANES, LANES)
            drawn = idx_ref[:, pl.ds(base, LANES)]
            mine = lax.broadcasted_iota(jnp.int32, (fits, LANES), 0) == fit
            offset = jnp.sum(jnp.where(mine, drawn, 0), axis=0, keepdims=True) - start
            column = base + lax.broadcasted_iota(jnp.int32, (1, LANES), 1)
            inside = (offset >= 0) & (offset < local_len) & (column < size)
            offset = jnp.broadcast_to(jnp.where(inside, offset, -1), (rows, LANES))
            high = offset >> 7
            low = offset & (LANES - 1)
            picked = jnp.full((rows, LANES), FAR, jnp.float32)
            for block in range(local_len // LANES):
                scored = s_ref[layer, :, block * LANES : (block + 1) * LANES]
                found = jnp.take_along_axis(scored, low, axis=1, mode="promise_in_bounds")
                picked = jnp.where(high == block, found, picked)
            g_ref[:, pl.ds(base, LANES)] = picked
            return jnp.maximum(top, jnp.max(picked, axis=1, keepdims=True))

        top = lax.fori_loop(
            0,
            capacity // LANES,
            one_tile,
            jnp.full((rows, 1), FAR, jnp.float32),
            unroll=8 if rows <= 64 else 1,
        )
        top = jnp.ceil(top)
        picked = g_ref[...]
        return jnp.where(picked > 0.5 * FAR, jnp.exp2(picked - top), 0.0), top

    parts = []
    for step in range(1, groups):
        peer = lax.rem(me + step, groups)
        parts.append(
            send(
                part.at[peer], part_in.at[step],
                send_part.at[step], recv_part.at[step], "seq", peer,
            )
        )
        parts[-1].start()
    part_in[0] = part[me]

    def column_of(j):
        return lax.rem(outer + 1 + j, outers) if exact else jnp.int32(j)

    across = []
    for j in range(half):
        expo, top = produce(column_of(j) * PAIR + 1 - inner)
        e_out[j] = joined_exponent(expo, top, lane)
        across.append(
            send(e_out.at[j], e_in.at[j], send_e.at[j], recv_e.at[j], "seq", partner)
        )
        if j > 0:
            across[j - 1].start()

    for copy in parts:
        copy.wait_recv()
    peak = part_in[0, 1][:, 64:65]
    for step in range(1, groups):
        peak = jnp.maximum(peak, part_in[step, 1][:, 64:65])
    numer, total = 0.0, 0.0
    for step in range(groups):
        factor = jnp.exp2(part_in[step, 1][:, 64:65] - peak)
        numer = numer + part_in[step, 0] * factor
        total = total + part_in[step, 1][:, 0:1] * factor
    merged = numer / total
    chunk_mine[...] = merged
    chunks[me] = merged
    across[half - 1].start()

    down, spread = [], []
    for j in range(half):
        dest = column_of(j)
        expo, top = produce(dest * PAIR + inner)
        if j == 0:
            for step in range(1, groups):
                peer = lax.rem(me + step, groups)
                spread.append(
                    send(
                        chunk_mine, chunks.at[me],
                        send_chunk.at[step], recv_chunk.at[step], "seq", peer,
                    )
                )
                spread[-1].start()
        across[j].wait_recv()
        other, other_top = split_exponent(e_in[j], capacity)
        both = jnp.maximum(top, other_top)
        expo = expo * jnp.exp2(top - both) + other * jnp.exp2(other_top - both)
        block = joined_exponent(expo, both, lane)
        copy = send(
            z_out.at[j], z_in.at[outer], send_z.at[j], recv_z.at[outer],
            "seq", dest * PAIR + inner,
        )
        down.append((dest, copy))
        if exact:
            if j == half - 1:
                z_in[outer] = block
            else:
                z_out[j] = block
                copy.start()
        else:
            z_out[j] = block
            pl.when(dest != outer)(copy.start)

            @pl.when(dest == outer)
            def _():
                z_in[outer] = block

    def only(condition, act):
        if exact:
            act()
        else:
            pl.when(condition)(act)

    def source_z(step):
        source = lax.rem(outer + step, outers)
        return source, send(
            z_out.at[0], z_in.at[source], send_z.at[0], recv_z.at[source], "seq", partner
        )

    def gave_p(step, target):
        return send(
            p_mine, p_all.at[fit_mine], send_p.at[step], recv_p.at[outer],
            "seq", target * PAIR + inner,
        )

    def came_p(source):
        fit = jnp.minimum(source, half - 1) * PAIR + inner
        arrival = send(
            p_mine, p_all.at[fit], send_p.at[0], recv_p.at[source], "seq", partner
        )
        onward = send(
            p_all.at[fit], p_all.at[fit], send_f.at[source], recv_f.at[source], "seq", partner
        )
        return arrival, onward

    def back_p(source):
        fit = jnp.minimum(source, half - 1) * PAIR + 1 - inner
        return send(
            p_mine, p_all.at[fit], send_f.at[source], recv_f.at[source], "seq", partner
        )

    gifts = [gave_p(step, lax.rem(outer + step, outers)) for step in range(1, outers)]
    own_onward = send(
        p_mine, p_all.at[fit_mine], send_f.at[outer], recv_f.at[outer], "seq", partner
    )
    results = [
        send(
            x_mine, x_all.at[fit_mine], send_x.at[step], recv_x.at[step],
            "seq", lax.rem(me + step, groups),
        )
        for step in range(1, groups)
    ]

    def near_first(step):
        if outers != 4:
            return lax.rem(outer + outers - step, outers)
        low, high = lax.rem(outer, 2), outer // 2
        flipped_low = 1 - low if step % 2 else low
        flipped_high = 1 - high if step // 2 else high
        return flipped_high * 2 + flipped_low

    def relay():
        for step in range(1, outers):
            source = near_first(step)
            arrival, onward = came_p(source)

            def pass_on():
                arrival.wait_recv()
                onward.start()

            only(source < half, pass_on)

    for copy in spread:
        copy.wait_recv()

    def work():
        for step in range(1, outers):
            source_z(step)[1].wait_recv()
        blocks = [split_exponent(z_in[source], capacity) for source in range(outers)]
        top = blocks[0][1]
        for _, other in blocks[1:]:
            top = jnp.maximum(top, other)
        probs = 0.0
        for expo, other in blocks:
            probs = probs + expo * jnp.exp2(other - top)
        probs = (probs / jnp.sum(probs, axis=1, keepdims=True)).astype(jnp.bfloat16)
        p_mine[...] = probs
        p_all[fit_mine] = probs
        gram = lax.dot_general(probs, probs, NT, preferred_element_type=jnp.float32)
        for copy in gifts:
            copy.start()
        own_onward.start()
        diagonal = lax.broadcasted_iota(jnp.int32, (rows, rows), 0) == lax.broadcasted_iota(
            jnp.int32, (rows, rows), 1
        )
        trace = jnp.sum(jnp.where(diagonal, gram, 0.0))
        ridge = RIDGE * trace / sizes_ref[0, fit_mine].astype(jnp.float32)
        span = rows // chunk
        base = (fit_mine // FITS_LAYER) * span
        target = jnp.concatenate([chunks[base + at] for at in range(span)], axis=0)
        target = target.astype(jnp.bfloat16).astype(jnp.float32)
        solved = solve_rows(jnp.where(diagonal, gram + ridge, gram), target)
        x_mine[...] = solved
        x_all[fit_mine] = solved
        for copy in results:
            copy.start()

    only(outer < half, work)
    relay()
    for copy in first + second + parts + spread + across:
        copy.wait_send()
    for j in range(half):
        dest, copy = down[j]
        if exact:
            if j < half - 1:
                copy.wait_send()
        else:
            pl.when(dest != outer)(copy.wait_send)
    for step in range(1, outers):
        source = lax.rem(outer + outers - step, outers)
        only(outer < half, gifts[step - 1].wait_send)
        only(source < half, came_p(source)[1].wait_send)
    only(outer < half, own_onward.wait_send)
    for source in range(half):
        back_p(source).wait_recv()
    for step in range(1, groups):
        source = lax.rem(me + groups - step, groups)
        only(source < fits, results[step - 1].wait_recv)
        only(outer < half, results[step - 1].wait_send)
    p_ref[...] = p_all[...]
    x_ref[...] = x_all[...]


def place_kernel(owners_ref, p_ref, x_ref, out_ref, probs_in, rows_in, placed, take, put):
    me = lax.axis_index("seq")
    fits = p_ref.shape[0]
    count = jnp.int32(0)
    chosen = [jnp.int32(0)] * SLOTS
    for fit in range(fits):
        mine = owners_ref[0, fit] == me
        for slot in range(SLOTS):
            chosen[slot] = jnp.where(mine & (count == slot), fit, chosen[slot])
        count = count + mine.astype(jnp.int32)
    takes, puts = [], []
    for slot in range(SLOTS):
        takes.append(
            [
                pltpu.make_async_copy(p_ref.at[chosen[slot]], probs_in.at[slot], take.at[0, slot]),
                pltpu.make_async_copy(x_ref.at[chosen[slot]], rows_in.at[slot], take.at[1, slot]),
            ]
        )
        for copy in takes[slot]:
            copy.start()
    for slot in range(SLOTS):
        for copy in takes[slot]:
            copy.wait()
        probs = probs_in[slot]
        rows = rows_in[slot]
        high = rows.astype(jnp.bfloat16)
        low = (rows - high.astype(jnp.float32)).astype(jnp.bfloat16)
        fitted = lax.dot_general(
            jnp.concatenate([probs, probs], axis=0),
            jnp.concatenate([high, low], axis=0),
            TN,
            preferred_element_type=jnp.float32,
        )
        placed[slot] = jnp.where(count > slot, fitted, 0.0).astype(jnp.bfloat16)
        puts.append(pltpu.make_async_copy(placed.at[slot], out_ref.at[0, slot], put.at[slot]))
        if slot > 0:
            puts[slot - 1].start()
    puts[SLOTS - 1].start()
    for copy in puts:
        copy.wait()


VMEM = pl.BlockSpec(memory_space=pltpu.VMEM)
ANY = pl.BlockSpec(memory_space=pl.ANY)
SMEM = pl.BlockSpec(memory_space=pltpu.SMEM)
PARAMS = dict(vmem_limit_bytes=60 * 1024 * 1024)


def on_device(queries, keys, values, indices, sizes, owners):
    layers, heads, count, width = queries.shape
    groups = lax.axis_size("seq")
    rows = groups * heads * count
    local_len = keys.shape[2]
    fits, capacity = indices.shape[1:]
    dma = pltpu.SemaphoreType.DMA
    outers, half = groups // PAIR, fits // PAIR
    chunk = layers * rows // groups
    packed = (rows, capacity + LANES)
    probs, solved = pl.pallas_call(
        fit_kernel,
        out_shape=(
            jax.ShapeDtypeStruct((fits, rows, capacity), jnp.bfloat16),
            jax.ShapeDtypeStruct((fits, rows, width), jnp.float32),
        ),
        in_specs=[SMEM, VMEM, ANY, ANY, VMEM],
        out_specs=(VMEM, VMEM),
        scratch_shapes=[
            pltpu.VMEM((heads, SUBLANES, width), jnp.float32),
            pltpu.VMEM((heads * SUBLANES, width), jnp.float32),
            pltpu.VMEM((rows * SUBLANES, width), jnp.float32),
            pltpu.VMEM((layers, local_len, width), jnp.bfloat16),
            pltpu.VMEM((layers, local_len, width), jnp.bfloat16),
            pltpu.VMEM((layers, rows, local_len), jnp.float32),
            pltpu.VMEM((rows, capacity), jnp.float32),
            pltpu.VMEM((groups, 2, chunk, width), jnp.float32),
            pltpu.VMEM((groups, 2, chunk, width), jnp.float32),
            pltpu.VMEM((chunk, width), jnp.float32),
            pltpu.VMEM((groups, chunk, width), jnp.float32),
            pltpu.VMEM((half,) + packed, jnp.bfloat16),
            pltpu.VMEM((half,) + packed, jnp.bfloat16),
            pltpu.VMEM((half,) + packed, jnp.bfloat16),
            pltpu.VMEM((outers,) + packed, jnp.bfloat16),
            pltpu.VMEM((rows, capacity), jnp.bfloat16),
            pltpu.VMEM((fits, rows, capacity), jnp.bfloat16),
            pltpu.VMEM((rows, width), jnp.float32),
            pltpu.VMEM((fits, rows, width), jnp.float32),
            dma((2,)),
            dma((heads,)),
            dma((heads,)),
            dma((groups,)),
            dma((groups,)),
            dma((groups,)),
            dma((groups,)),
            dma((groups,)),
            dma((groups,)),
            dma((half,)),
            dma((half,)),
            dma((half,)),
            dma((outers,)),
            dma((outers,)),
            dma((outers,)),
            dma((outers,)),
            dma((outers,)),
            dma((groups,)),
            dma((groups,)),
        ],
        compiler_params=pltpu.CompilerParams(collective_id=2, has_side_effects=True, **PARAMS),
    )(
        sizes,
        queries.reshape(layers * heads, width),
        keys[:, 0],
        values[:, 0],
        indices[0],
    )
    return pl.pallas_call(
        place_kernel,
        out_shape=jax.ShapeDtypeStruct((1, SLOTS, capacity, width), jnp.bfloat16),
        in_specs=[SMEM, ANY, ANY],
        out_specs=ANY,
        scratch_shapes=[
            pltpu.VMEM((SLOTS, rows, capacity), jnp.bfloat16),
            pltpu.VMEM((SLOTS, rows, width), jnp.float32),
            pltpu.VMEM((SLOTS, capacity, width), jnp.bfloat16),
            dma((2, SLOTS)),
            dma((SLOTS,)),
        ],
        compiler_params=pltpu.CompilerParams(**PARAMS),
    )(owners, probs, solved)


def solution(mesh):
    in_specs = (
        P(None, None, ("head", "seq"), None),
        P(None, "head", "seq", None),
        P(None, "head", "seq", None),
        P("head", None, None),
        P("head", None),
        P("head", None),
    )
    out_specs = P("head", "seq", None, None)
    return jax.shard_map(
        on_device, mesh=mesh, in_specs=in_specs, out_specs=out_specs, check_vma=False
    )
```
